8 devices in a mesh: data: 1 (over z), model: 2 (over y), seq: 4 (over x, core).
Axes of the slice: x: 2, y: 2, z: 1, core: 2. Of those that a mesh axis runs over, the one named last changes fastest.
Arguments:
- tokens: bfloat16 [64, 2048, 1280], P('data', 'seq')
- lengths: int32 [64], P('data')
- slot_params: bfloat16 [1280, 128], replicated
- logit_scale: float32 [], replicated
- w_in: bfloat16 [32, 1280, 5120], P('seq', None, 'model')
- w_out: bfloat16 [32, 5120, 1280], P('seq', 'model')
Outputs:
- output: bfloat16 [64, 2048, 1280], P('data', 'seq')
All inputs are finite; a program needn't handle non-finite values.
Results may differ from the reference program's by a relative error of at most 0.0143614.
Values are sent between devices in bfloat16 or wider.
A program may use at most 1.25 GiB of HBM per device.

```python
import math
import jax
import jax.numpy as jnp
from jax import lax

BATCH_SIZE = 64
SEQ_LEN = 2048
MODEL_DIM = 1280
HIDDEN_DIM = 5120
NUM_EXPERTS = 32
EXPERT_SLOTS = 4
NUM_SLOTS_TOTAL = NUM_EXPERTS * EXPERT_SLOTS
NORM_EPS = 1e-6


def setup_inputs(seed: int = 0, part: int = 0) -> dict:
    root_key = jax.random.key(seed)
    key_phi, key_gain, key_win, key_wout, key_part = jax.random.split(root_key, 5)
    part_key = jax.random.fold_in(key_part, part)
    key_tok, key_len = jax.random.split(part_key, 2)
    tokens = jax.random.normal(key_tok, (BATCH_SIZE, SEQ_LEN, MODEL_DIM), jnp.float32).astype(jnp.bfloat16)
    drawn = jax.random.randint(key_len, (BATCH_SIZE,), SEQ_LEN // 4, SEQ_LEN + 1, jnp.int32)
    lengths = jnp.where(jnp.arange(BATCH_SIZE) == 0, SEQ_LEN, drawn).astype(jnp.int32)
    slot_params = jax.random.normal(key_phi, (MODEL_DIM, NUM_SLOTS_TOTAL), jnp.float32).astype(jnp.bfloat16)
    logit_scale = math.sqrt(MODEL_DIM) * jax.random.uniform(key_gain, (), jnp.float32, 1.0, 2.0)
    in_scale = math.sqrt(SEQ_LEN) / (4.0 * math.sqrt(MODEL_DIM))
    w_in = (jax.random.normal(key_win, (NUM_EXPERTS, MODEL_DIM, HIDDEN_DIM), jnp.float32) * in_scale).astype(jnp.bfloat16)
    w_out = (jax.random.normal(key_wout, (NUM_EXPERTS, HIDDEN_DIM, MODEL_DIM), jnp.float32) / math.sqrt(HIDDEN_DIM)).astype(jnp.bfloat16)
    return {"tokens": tokens, "lengths": lengths, "slot_params": slot_params, "logit_scale": logit_scale, "w_in": w_in, "w_out": w_out}


def unit_vectors(values, axis):
    v32 = values.astype(jnp.float32)
    return (v32 * lax.rsqrt(jnp.sum(v32 * v32, axis=axis, keepdims=True) + NORM_EPS)).astype(jnp.bfloat16)


def reference(tokens, lengths, slot_params, logit_scale, w_in, w_out):
    slot_unit = unit_vectors(slot_params, 0)
    positions = jnp.arange(SEQ_LEN)

    def seq_logits(seq_tokens):
        return logit_scale * jnp.dot(unit_vectors(seq_tokens, 1), slot_unit, preferred_element_type=jnp.float32)

    def dispatch(args):
        seq_tokens, seq_length = args
        logits = seq_logits(seq_tokens)
        masked = jnp.where((positions < seq_length)[:, None], logits, -1e30)
        weights = jnp.exp(masked - jnp.max(masked, axis=0, keepdims=True))
        col_sum = jnp.sum(weights, axis=0)
        slot_sum = jnp.dot(weights.astype(jnp.bfloat16).T, seq_tokens, preferred_element_type=jnp.float32)
        return (slot_sum / col_sum[:, None]).astype(jnp.bfloat16)

    slot_in = lax.map(dispatch, (tokens, lengths))
    per_expert = slot_in.reshape(BATCH_SIZE, NUM_EXPERTS, EXPERT_SLOTS, MODEL_DIM).transpose(1, 0, 2, 3).reshape(NUM_EXPERTS, BATCH_SIZE * EXPERT_SLOTS, MODEL_DIM)

    def expert_ffn(args):
        rows, first, second = args
        hidden = jax.nn.gelu(jnp.dot(rows, first, preferred_element_type=jnp.float32), approximate=False).astype(jnp.bfloat16)
        return jnp.dot(hidden, second, preferred_element_type=jnp.float32).astype(jnp.bfloat16)

    expert_out = lax.map(expert_ffn, (per_expert, w_in, w_out))
    slot_out = expert_out.reshape(NUM_EXPERTS, BATCH_SIZE, EXPERT_SLOTS, MODEL_DIM).transpose(1, 0, 2, 3).reshape(BATCH_SIZE, NUM_SLOTS_TOTAL, MODEL_DIM)

    def combine(args):
        seq_tokens, seq_length, seq_slots = args
        mix_weights = jax.nn.softmax(seq_logits(seq_tokens), axis=1).astype(jnp.bfloat16)
        mixed = jnp.dot(mix_weights, seq_slots, preferred_element_type=jnp.float32)
        return jnp.where((positions < seq_length)[:, None], mixed, 0.0).astype(jnp.bfloat16)

    return lax.map(combine, (tokens, lengths, slot_out))
```

```python
import functools

import jax
import jax.numpy as jnp
from jax import lax
from jax.experimental import pallas as pl
from jax.experimental.pallas import tpu as pltpu
from jax.sharding import PartitionSpec as P


NORM_EPS = 1e-6
NEG = -1e30
MESH = pl.DeviceIdType.MESH
CHUNK_SEQS = 4
X_SLOTS = 6
C_SLOTS = 8
ROW_BLOCK = 256
HIDDEN_TILE = 2560
SUB_TILE = 256
LANES = 128
GROUPS = 2
BATCH_CHUNKS = 4
COMBINE_SEQS = 4


def dispatch_kernel(n_half, n_tok, dim, n_slots, per_dev, phi_ref, len_ref, g_ref, x_hbm, xs_hbm, c_hbm,
                    v_ref, xbuf, lbuf, cbuf, sbuf, lse1, r1, lr1, m0, s2, lse2, r2, lr2, xso,
                    xsem, csem, osem, s1_sem, r1_sem, s2_sem, r2_sem, s3_sem, r3_sem):
    s = lax.axis_index("seq")
    m = lax.axis_index("model")
    core_peer = {"seq": s + 1 - 2 * lax.rem(s, 2)}
    x_peer = {"seq": lax.rem(s + 2, 4)}
    y_peer = {"model": 1 - m}
    cs = CHUNK_SEQS
    n = n_half // cs

    barrier = pltpu.get_barrier_semaphore()
    for peer in (core_peer, x_peer, y_peer):
        pl.semaphore_signal(barrier, inc=1, device_id=peer, device_id_type=MESH)

    def batch_of(t):
        return lax.rem(m * n_half + t, 2 * n_half)

    def x_copy(t):
        slot = lax.rem(t, X_SLOTS)
        return pltpu.make_async_copy(x_hbm.at[batch_of(t)], xbuf.at[slot], xsem.at[slot])

    def c_copy(t):
        slot = lax.rem(t, C_SLOTS)
        return pltpu.make_async_copy(cbuf.at[slot], c_hbm.at[batch_of(t)], csem.at[slot])

    for t in range(X_SLOTS - 1):
        x_copy(t).start()

    phi = phi_ref[...].astype(jnp.float32)
    unit = (phi * lax.rsqrt(jnp.sum(phi * phi, axis=0, keepdims=True) + NORM_EPS)).astype(jnp.bfloat16)
    row = lax.broadcasted_iota(jnp.int32, (n_slots, n_slots), 0)
    col = lax.broadcasted_iota(jnp.int32, (n_slots, n_slots), 1)
    target = jnp.bitwise_xor(col, s * per_dev)
    pick = jnp.where(row == target, 1.0, 0.0).astype(jnp.bfloat16)
    v_ref[...] = jnp.dot(unit, pick, preferred_element_type=jnp.float32).astype(jnp.bfloat16)
    lse1[...] = jnp.zeros_like(lse1)
    g = g_ref[0]

    pl.semaphore_wait(barrier, 3)

    def logits_and_mix(t):
        xslot = lax.rem(t, X_SLOTS)
        cslot = lax.rem(t, C_SLOTS)
        length = len_ref[batch_of(t)]

        @pl.when(t + X_SLOTS - 1 < 2 * n_half)
        def _():
            x_copy(t + X_SLOTS - 1).start()

        x_copy(t).wait()

        @pl.when(t >= C_SLOTS)
        def _():
            c_copy(t - C_SLOTS).wait()

        dots = jnp.dot(xbuf[xslot], v_ref[...], preferred_element_type=jnp.float32)
        for r in range(n_tok // ROW_BLOCK):
            rows = pl.ds(r * ROW_BLOCK, ROW_BLOCK)
            square = jnp.zeros((ROW_BLOCK, LANES), jnp.float32)
            for c in range(dim // LANES):
                x32 = xbuf[xslot, rows, c * LANES:(c + 1) * LANES].astype(jnp.float32)
                square += x32 * x32
            scale = lax.rsqrt(jnp.sum(square, axis=1, keepdims=True) + NORM_EPS)
            block = dots[r * ROW_BLOCK:(r + 1) * ROW_BLOCK]
            lg = jnp.where(scale > 0.0, block * (g * scale), 0.0)
            lbuf[rows, :] = lg
            e = jnp.exp(lg - jnp.max(lg, axis=1, keepdims=True))
            mix = e * (1.0 / jnp.sum(e, axis=1, keepdims=True))
            pos = s * n_tok + r * ROW_BLOCK + lax.broadcasted_iota(jnp.int32, (ROW_BLOCK, 1), 0)
            cbuf[cslot, rows, :] = jnp.where(pos < length, mix, 0.0).astype(jnp.bfloat16)
        c_copy(t).start()
        return xslot, length

    def own(k, j):
        t = k * cs + j
        xslot, length = logits_and_mix(t)
        ok = s * n_tok + lax.broadcasted_iota(jnp.int32, (n_tok, 1), 0) < length
        lg = jnp.where(ok, lbuf[...], NEG)
        mx = jnp.max(lg, axis=0, keepdims=True)
        w = jnp.where(ok, jnp.exp(lg - mx), 0.0)
        z = jnp.sum(w, axis=0, keepdims=True)
        z = jnp.where(z > 0.0, z, 1.0)
        lse1[k, pl.ds(j, 1), :] = mx + jnp.log(z)
        rz = jnp.transpose(jnp.broadcast_to(1.0 / z, (8, n_slots)))[:, :1]
        part = lax.dot_general(w.astype(jnp.bfloat16), xbuf[xslot], (((0,), (0,)), ((), ())), preferred_element_type=jnp.float32)
        sbuf[t] = (part * rz).astype(jnp.bfloat16)

    def remote(src, dst, send, recv, peer):
        return pltpu.make_async_remote_copy(src, dst, send, recv, device_id=peer, device_id_type=MESH)

    def d1(k):
        seqs = pl.ds(k * cs, cs)
        p = per_dev
        return (
            remote(sbuf.at[seqs, pl.ds(p, p)], r1.at[seqs, pl.ds(0, p)], s1_sem.at[k, 0], r1_sem.at[k, 0], core_peer),
            remote(sbuf.at[seqs, pl.ds(3 * p, p)], r1.at[seqs, pl.ds(p, p)], s1_sem.at[k, 1], r1_sem.at[k, 1], core_peer),
            remote(lse1.at[k], lr1.at[k], s1_sem.at[k, 2], r1_sem.at[k, 2], core_peer),
        )

    def d2(k):
        seqs = pl.ds(k * cs, cs)
        return (
            remote(s2.at[seqs], r2.at[seqs], s2_sem.at[k, 0], r2_sem.at[k, 0], x_peer),
            remote(lse2.at[k], lr2.at[k], s2_sem.at[k, 1], r2_sem.at[k, 1], x_peer),
        )

    def d3(k):
        seqs = pl.ds(k * cs, cs)
        return remote(xso.at[seqs], xs_hbm.at[pl.ds(m * n_half + k * cs, cs)], s3_sem.at[k], r3_sem.at[k], y_peer)

    def keep(k):
        seqs = pl.ds(k * cs, cs)
        return pltpu.make_async_copy(xso.at[seqs], xs_hbm.at[pl.ds(m * n_half + k * cs, cs)], osem.at[k])

    def weights(a, b):
        top = jnp.maximum(a, b)
        ea, eb = jnp.exp(a - top), jnp.exp(b - top)
        tot = ea + eb
        return jnp.transpose(ea / tot), jnp.transpose(eb / tot), top + jnp.log(tot)

    def merge1(k):
        for c in d1(k):
            c.wait_recv()
        p = per_dev
        wa, wb, joint = weights(lse1[k], pltpu.roll(lr1[k], n_slots - p, 1))
        lse2[k] = joint
        for j in range(cs):
            t = k * cs + j
            m0[t] = wa[:p, j:j + 1] * sbuf[t, 0:p, :].astype(jnp.float32) + wb[:p, j:j + 1] * r1[t, 0:p, :].astype(jnp.float32)
            s2[t] = (wa[2 * p:3 * p, j:j + 1] * sbuf[t, 2 * p:3 * p, :].astype(jnp.float32)
                     + wb[2 * p:3 * p, j:j + 1] * r1[t, p:2 * p, :].astype(jnp.float32)).astype(jnp.bfloat16)
        for c in d2(k):
            c.start()

    def merge2(k):
        for c in d2(k):
            c.wait_recv()
        p = per_dev
        wa, wb, _ = weights(lse2[k], pltpu.roll(lr2[k], n_slots - 2 * p, 1))
        for j in range(cs):
            t = k * cs + j
            xso[t] = (wa[:p, j:j + 1] * m0[t] + wb[:p, j:j + 1] * r2[t].astype(jnp.float32)).astype(jnp.bfloat16)
        d3(k).start()
        keep(k).start()

    lead = 4
    early = n - lead
    late = n // 2 - 1

    @pl.loop(0, 2 * n)
    def _(k):
        @pl.when(k < n)
        def _():
            @pl.loop(0, cs)
            def _(j):
                own(k, j)

            for c in d1(k):
                c.start()

        @pl.when(k >= n)
        def _():
            @pl.loop(0, cs)
            def _(j):
                logits_and_mix(k * cs + j)

        @pl.when((k >= 1) & (k <= n))
        def _():
            merge1(k - 1)

        @pl.when((k >= lead) & (k < n))
        def _():
            merge2(k - lead)

        @pl.when((k > n) & (lax.rem(k - n, 2) == 1) & ((k - n) // 2 < late))
        def _():
            merge2(early + (k - n) // 2)

    @pl.loop(early + late, n)
    def _(k):
        merge2(k)

    @pl.loop(2 * n_half - C_SLOTS, 2 * n_half)
    def _(t):
        c_copy(t).wait()

    @pl.loop(0, n)
    def _(k):
        for c in d1(k):
            c.wait_send()
        for c in d2(k):
            c.wait_send()
        d3(k).wait()
        keep(k).wait()


def dispatch(tokens, lengths, phi, scale, per_dev):
    batch, n_tok, dim = tokens.shape
    n_slots = phi.shape[1]
    half = batch // 2
    n = half // CHUNK_SEQS
    bf, f32 = jnp.bfloat16, jnp.float32
    return pl.pallas_call(
        functools.partial(dispatch_kernel, half, n_tok, dim, n_slots, per_dev),
        out_shape=(jax.ShapeDtypeStruct((batch, per_dev, dim), bf), jax.ShapeDtypeStruct((batch, n_tok, n_slots), bf)),
        in_specs=[
            pl.BlockSpec(memory_space=pltpu.VMEM),
            pl.BlockSpec(memory_space=pltpu.SMEM),
            pl.BlockSpec(memory_space=pltpu.SMEM),
            pl.BlockSpec(memory_space=pl.ANY),
        ],
        out_specs=[pl.BlockSpec(memory_space=pl.ANY)] * 2,
        scratch_shapes=[
            pltpu.VMEM((dim, n_slots), bf),
            pltpu.VMEM((X_SLOTS, n_tok, dim), bf),
            pltpu.VMEM((n_tok, n_slots), f32),
            pltpu.VMEM((C_SLOTS, n_tok, n_slots), bf),
            pltpu.VMEM((half, n_slots, dim), bf),
            pltpu.VMEM((n, 8, n_slots), f32),
            pltpu.VMEM((half, 2 * per_dev, dim), bf),
            pltpu.VMEM((n, 8, n_slots), f32),
            pltpu.VMEM((half, per_dev, dim), f32),
            pltpu.VMEM((half, per_dev, dim), bf),
            pltpu.VMEM((n, 8, n_slots), f32),
            pltpu.VMEM((half, per_dev, dim), bf),
            pltpu.VMEM((n, 8, n_slots), f32),
            pltpu.VMEM((half, per_dev, dim), bf),
            pltpu.SemaphoreType.DMA((X_SLOTS,)),
            pltpu.SemaphoreType.DMA((C_SLOTS,)),
            pltpu.SemaphoreType.DMA((n,)),
            pltpu.SemaphoreType.DMA((n, 3)),
            pltpu.SemaphoreType.DMA((n, 3)),
            pltpu.SemaphoreType.DMA((n, 2)),
            pltpu.SemaphoreType.DMA((n, 2)),
            pltpu.SemaphoreType.DMA((n,)),
            pltpu.SemaphoreType.DMA((n,)),
        ],
        compiler_params=pltpu.CompilerParams(collective_id=0, has_side_effects=True, vmem_limit_bytes=58 * 1024 * 1024),
        name="dispatch",
    )(phi, lengths, scale, tokens)


def ffn_kernel(first, batch, slot_per, per_dev, grp, x_ref, wi_ref, wo_ref, *rest):
    outs, (xf, xe, acc, og) = rest[:BATCH_CHUNKS], rest[BATCH_CHUNKS:]
    e, h = pl.program_id(0), pl.program_id(1)
    last_e, last_h = pl.num_programs(0) - 1, pl.num_programs(1) - 1
    tiles = x_ref.shape[2] // LANES

    @pl.when((e == 0) & (h == 0))
    def _():
        @pl.loop(0, batch)
        def _(b):
            rows = pl.ds(pl.multiple_of(b * per_dev, per_dev), per_dev)
            for c in range(tiles):
                xf[c, rows, :] = x_ref[b, :, c * LANES:(c + 1) * LANES].astype(jnp.float32)

    @pl.when(h == 0)
    def _():
        for q in range(slot_per):
            for c in range(tiles):
                rows = xf[c, pl.ds((first + e) * slot_per + q, batch, stride=per_dev), :]
                xe[q * batch:(q + 1) * batch, c * LANES:(c + 1) * LANES] = rows.astype(jnp.bfloat16)

    acts = []
    for i in range(wi_ref.shape[2] // SUB_TILE):
        hid = jnp.dot(xe[...], wi_ref[0, :, i * SUB_TILE:(i + 1) * SUB_TILE], preferred_element_type=jnp.float32)
        acts.append((0.5 * hid * (1.0 + lax.erf(hid * 0.7071067811865476))).astype(jnp.bfloat16))
    part = jnp.dot(jnp.concatenate(acts, axis=1), wo_ref[0], preferred_element_type=jnp.float32)

    @pl.when(h == 0)
    def _():
        acc[...] = part

    @pl.when(h > 0)
    def _():
        acc[...] += part

    @pl.when(h == last_h)
    def _():
        for q in range(slot_per):
            for c in range(tiles):
                og[c, pl.ds(e * slot_per + q, batch, stride=grp), :] = acc[q * batch:(q + 1) * batch, c * LANES:(c + 1) * LANES]

    @pl.when((e == last_e) & (h == last_h))
    def _():
        step = batch // BATCH_CHUNKS
        for i, out in enumerate(outs):
            for b in range(step):
                rows = slice((i * step + b) * grp, (i * step + b + 1) * grp)
                for c in range(tiles):
                    out[b, :, c * LANES:(c + 1) * LANES] = og[c, rows, :].astype(jnp.bfloat16)


def ffn(group, xs, w_in, w_out, slot_per):
    batch, per_dev, dim = xs.shape
    experts, _, hidden = w_in.shape
    ge = experts // GROUPS
    grp = ge * slot_per
    first = group * ge
    step = batch // BATCH_CHUNKS
    rows = batch * slot_per
    return pl.pallas_call(
        functools.partial(ffn_kernel, first, batch, slot_per, per_dev, grp),
        grid=(ge, hidden // HIDDEN_TILE),
        out_shape=[jax.ShapeDtypeStruct((step, grp, dim), jnp.bfloat16)] * BATCH_CHUNKS,
        in_specs=[
            pl.BlockSpec((batch, per_dev, dim), lambda e, h: (0, 0, 0)),
            pl.BlockSpec((1, dim, HIDDEN_TILE), lambda e, h: (first + e, 0, h)),
            pl.BlockSpec((1, HIDDEN_TILE, dim), lambda e, h: (first + e, h, 0)),
        ],
        out_specs=[pl.BlockSpec((step, grp, dim), lambda e, h: (0, 0, 0))] * BATCH_CHUNKS,
        scratch_shapes=[
            pltpu.VMEM((dim // LANES, batch * per_dev, LANES), jnp.float32),
            pltpu.VMEM((rows, dim), jnp.bfloat16),
            pltpu.VMEM((rows, dim), jnp.float32),
            pltpu.VMEM((dim // LANES, batch * grp, LANES), jnp.float32),
        ],
        compiler_params=pltpu.CompilerParams(dimension_semantics=("arbitrary", "arbitrary"), vmem_limit_bytes=58 * 1024 * 1024),
        cost_estimate=pl.CostEstimate(flops=4 * ge * rows * dim * hidden, bytes_accessed=4 * ge * dim * hidden, transcendentals=0),
        name="ffn",
    )(xs, w_in, w_out)


def combine_kernel(first, n_tok, n_pieces, len_ref, off_ref, c_ref, *rest):
    pieces, out_ref = rest[:n_pieces], rest[-1]
    pos = off_ref[0] + lax.broadcasted_iota(jnp.int32, (n_tok, 1), 0)
    for i in range(COMBINE_SEQS):
        slots = jnp.concatenate([p[i] for p in pieces], axis=0)
        mixed = jnp.dot(c_ref[i], slots, preferred_element_type=jnp.float32)
        ok = pos < len_ref[first + pl.program_id(0) * COMBINE_SEQS + i]
        out_ref[i] = jnp.where(ok, mixed, 0.0).astype(jnp.bfloat16)


def combine(chunk, mix, pieces, lengths, offset, y):
    batch, n_tok, n_slots = mix.shape
    step, grp, dim = pieces[0].shape
    first = chunk * step
    n_p = len(pieces)
    cs = COMBINE_SEQS
    base = first // cs
    in_specs = [
        pl.BlockSpec((cs, n_tok, n_slots), lambda b, *_: (base + b, 0, 0)),
        *[pl.BlockSpec((cs, grp, dim), lambda b, *_: (b, 0, 0))] * n_p,
    ]
    args = [lengths, offset, mix, *pieces]
    alias = {}
    if y is not None:
        in_specs.append(pl.BlockSpec(memory_space=pl.ANY))
        args.append(y)
        alias = {len(args) - 1: 0}
    return pl.pallas_call(
        functools.partial(combine_kernel, first, n_tok, n_p),
        grid_spec=pltpu.PrefetchScalarGridSpec(
            num_scalar_prefetch=2,
            grid=(step // cs,),
            in_specs=in_specs,
            out_specs=pl.BlockSpec((cs, n_tok, dim), lambda b, *_: (base + b, 0, 0)),
        ),
        out_shape=jax.ShapeDtypeStruct((batch, n_tok, dim), jnp.bfloat16),
        input_output_aliases=alias,
        compiler_params=pltpu.CompilerParams(dimension_semantics=("arbitrary",), vmem_limit_bytes=32 * 1024 * 1024),
        cost_estimate=pl.CostEstimate(flops=2 * 2 * step * n_tok * n_slots * dim, bytes_accessed=2 * step * n_tok * (dim + n_slots), transcendentals=0),
        name="combine",
    )(*args)


def solution(mesh):
    seq_size = mesh.shape["seq"]
    swap_y = [(0, 1), (1, 0)]
    swap_x = [(i, i ^ 2) for i in range(seq_size)]
    swap_c = [(i, i ^ 1) for i in range(seq_size)]

    def local_layer(tokens, lengths, slot_params, logit_scale, w_in, w_out):
        n_tok = tokens.shape[1]
        per_dev = slot_params.shape[1] // seq_size
        slot_per = per_dev // w_in.shape[0]
        offset = (lax.axis_index("seq") * n_tok).reshape(1).astype(jnp.int32)
        xs, mix = dispatch(tokens, lengths, slot_params, logit_scale.reshape(1), per_dev)
        table = {}
        for group in range(GROUPS):
            parts = ffn(group, xs, w_in, w_out, slot_per)
            for k, part in enumerate(parts):
                other = lax.ppermute(part, "model", swap_y)
                own = (part.astype(jnp.float32) + other.astype(jnp.float32)).astype(jnp.bfloat16)
                across = lax.ppermute(own, "seq", swap_x)
                table[k, group, 0] = own
                table[k, group, 1] = lax.ppermute(own, "seq", swap_c)
                table[k, group, 2] = across
                table[k, group, 3] = lax.ppermute(across, "seq", swap_c)
        y = None
        for k in range(BATCH_CHUNKS):
            pieces = [table[k, group, q] for q in range(seq_size) for group in range(GROUPS)]
            y = combine(k, mix, pieces, lengths, offset, y)
        return y

    return jax.shard_map(local_layer, mesh=mesh, in_specs=(P("data", "seq", None), P("data"), P(), P(), P("seq", None, "model"), P("seq", "model", None)), out_specs=P("data", "seq", None), check_vma=False)
```

```python
import functools

import jax
import jax.numpy as jnp
from jax import lax
from jax.experimental import pallas as pl
from jax.experimental.pallas import tpu as pltpu
from jax.sharding import PartitionSpec as P


NORM_EPS = 1e-6
NEG = -1e30
MESH = pl.DeviceIdType.MESH
CHUNK_SEQS = 2
LEAD = 4
LATE_EVERY = 1
IN_DISPATCH = 16
MIX_CALLS = 2
MIX_SEQS = 2
X_SLOTS = 6
C_SLOTS = 8
ROW_BLOCK = 256
HIDDEN_TILE = 1280
LANES = 128
GROUPS = 4
CHUNKS = (2, 2, 2, 4)
MIX_CHUNKS = 4
COMBINE_SEQS = 4


def slot_units(phi, s, per_dev):
    n_slots = phi.shape[1]
    p32 = phi.astype(jnp.float32)
    unit = (p32 * lax.rsqrt(jnp.sum(p32 * p32, axis=0, keepdims=True) + NORM_EPS)).astype(jnp.bfloat16)
    row = lax.broadcasted_iota(jnp.int32, (n_slots, n_slots), 0)
    col = lax.broadcasted_iota(jnp.int32, (n_slots, n_slots), 1)
    pick = jnp.where(row == jnp.bitwise_xor(col, s * per_dev), 1.0, 0.0).astype(jnp.bfloat16)
    return jnp.dot(unit, pick, preferred_element_type=jnp.float32).astype(jnp.bfloat16)


def logit_block(x_ref, dots, g, r):
    rows = pl.ds(r * ROW_BLOCK, ROW_BLOCK)
    square = jnp.zeros((ROW_BLOCK, LANES), jnp.float32)
    for c in range(x_ref.shape[1] // LANES):
        x32 = x_ref[rows, c * LANES:(c + 1) * LANES].astype(jnp.float32)
        square += x32 * x32
    scale = lax.rsqrt(jnp.sum(square, axis=1, keepdims=True) + NORM_EPS)
    return jnp.where(scale > 0.0, dots[r * ROW_BLOCK:(r + 1) * ROW_BLOCK] * (g * scale), 0.0)


def mix_block(lg, first_pos, length):
    e = jnp.exp(lg - jnp.max(lg, axis=1, keepdims=True))
    mix = e * (1.0 / jnp.sum(e, axis=1, keepdims=True))
    pos = first_pos + lax.broadcasted_iota(jnp.int32, (lg.shape[0], 1), 0)
    return jnp.where(pos < length, mix, 0.0).astype(jnp.bfloat16)


def mix_kernel(per_dev, seqs, idx_ref, len_ref, phi_ref, g_ref, x_ref, _, c_ref, v_ref):
    s = idx_ref[0]
    i = pl.program_id(0)

    @pl.when(i == 0)
    def _():
        v_ref[...] = slot_units(phi_ref[...], s, per_dev)

    n_tok = x_ref.shape[1]
    for j in range(seqs):
        length = len_ref[(idx_ref[1] + i) * seqs + j]
        dots = jnp.dot(x_ref[j], v_ref[...], preferred_element_type=jnp.float32)
        for r in range(n_tok // ROW_BLOCK):
            lg = logit_block(x_ref.at[j], dots, g_ref[0], r)
            c_ref[j, r * ROW_BLOCK:(r + 1) * ROW_BLOCK, :] = mix_block(lg, s * n_tok + r * ROW_BLOCK, length)


def mix_weights(part, tokens, lengths, phi, scale, per_dev, mix):
    batch, n_tok, dim = tokens.shape
    n_slots = phi.shape[1]
    count = (batch // 2 - IN_DISPATCH) // MIX_CALLS
    seqs = MIX_SEQS
    start = lax.rem(lax.axis_index("model") * (batch // 2) + batch // 2 + IN_DISPATCH + part * count, batch)
    index = jnp.stack([lax.axis_index("seq"), start // seqs]).astype(jnp.int32)
    block = lambda i, idx, _: (idx[1] + i, 0, 0)
    return pl.pallas_call(
        functools.partial(mix_kernel, per_dev, seqs),
        grid_spec=pltpu.PrefetchScalarGridSpec(
            num_scalar_prefetch=2,
            grid=(count // seqs,),
            in_specs=[
                pl.BlockSpec((dim, n_slots), lambda i, *_: (0, 0)),
                pl.BlockSpec(memory_space=pltpu.SMEM),
                pl.BlockSpec((seqs, n_tok, dim), block),
                pl.BlockSpec(memory_space=pl.ANY),
            ],
            out_specs=pl.BlockSpec((seqs, n_tok, n_slots), block),
            scratch_shapes=[pltpu.VMEM((dim, n_slots), jnp.bfloat16)],
        ),
        out_shape=jax.ShapeDtypeStruct(mix.shape, mix.dtype),
        input_output_aliases={5: 0},
        compiler_params=pltpu.CompilerParams(dimension_semantics=("arbitrary",), vmem_limit_bytes=32 * 1024 * 1024),
        cost_estimate=pl.CostEstimate(flops=4 * count * n_tok * n_slots * dim, bytes_accessed=2 * count * n_tok * dim, transcendentals=0),
        name="mix",
    )(index, lengths, phi, scale, tokens, mix)


def dispatch_kernel(n_half, n_tok, n_slots, per_dev, phi_ref, len_ref, g_ref, x_hbm, xs_hbm, c_hbm,
                    v_ref, xbuf, lbuf, cbuf, sbuf, lse1, r1, lr1, m0, s2, lse2, r2, lr2, xso,
                    xsem, csem, osem, s1_sem, r1_sem, s2_sem, r2_sem, s3_sem, r3_sem):
    s = lax.axis_index("seq")
    m = lax.axis_index("model")
    core_peer = {"seq": s + 1 - 2 * lax.rem(s, 2)}
    x_peer = {"seq": lax.rem(s + 2, 4)}
    y_peer = {"model": 1 - m}
    cs = CHUNK_SEQS
    n = n_half // cs
    total = n_half + IN_DISPATCH
    steps = total // cs

    barrier = pltpu.get_barrier_semaphore()
    for peer in (core_peer, x_peer, y_peer):
        pl.semaphore_signal(barrier, inc=1, device_id=peer, device_id_type=MESH)

    def batch_of(t):
        return lax.rem(m * n_half + t, 2 * n_half)

    def x_copy(t):
        slot = lax.rem(t, X_SLOTS)
        return pltpu.make_async_copy(x_hbm.at[batch_of(t)], xbuf.at[slot], xsem.at[slot])

    def c_copy(t):
        slot = lax.rem(t, C_SLOTS)
        return pltpu.make_async_copy(cbuf.at[slot], c_hbm.at[batch_of(t)], csem.at[slot])

    for t in range(X_SLOTS - 1):
        x_copy(t).start()

    v_ref[...] = slot_units(phi_ref[...], s, per_dev)
    lse1[...] = jnp.zeros_like(lse1)
    g = g_ref[0]

    pl.semaphore_wait(barrier, 3)

    def logits_and_mix(t):
        xslot = lax.rem(t, X_SLOTS)
        cslot = lax.rem(t, C_SLOTS)
        length = len_ref[batch_of(t)]

        @pl.when(t + X_SLOTS - 1 < total)
        def _():
            x_copy(t + X_SLOTS - 1).start()

        x_copy(t).wait()

        @pl.when(t >= C_SLOTS)
        def _():
            c_copy(t - C_SLOTS).wait()

        dots = jnp.dot(xbuf[xslot], v_ref[...], preferred_element_type=jnp.float32)
        for r in range(n_tok // ROW_BLOCK):
            rows = pl.ds(r * ROW_BLOCK, ROW_BLOCK)
            lg = logit_block(xbuf.at[xslot], dots, g, r)
            lbuf[rows, :] = lg
            cbuf[cslot, rows, :] = mix_block(lg, s * n_tok + r * ROW_BLOCK, length)
        c_copy(t).start()
        return xslot, length

    def own(k, j):
        t = k * cs + j
        xslot, length = logits_and_mix(t)
        ok = s * n_tok + lax.broadcasted_iota(jnp.int32, (n_tok, 1), 0) < length
        lg = jnp.where(ok, lbuf[...], NEG)
        mx = jnp.max(lg, axis=0, keepdims=True)
        w = jnp.where(ok, jnp.exp(lg - mx), 0.0)
        z = jnp.sum(w, axis=0, keepdims=True)
        z = jnp.where(z > 0.0, z, 1.0)
        lse1[k, pl.ds(j, 1), :] = mx + jnp.log(z)
        rz = jnp.transpose(jnp.broadcast_to(1.0 / z, (8, n_slots)))[:, :1]
        part = lax.dot_general(w.astype(jnp.bfloat16), xbuf[xslot], (((0,), (0,)), ((), ())), preferred_element_type=jnp.float32)
        sbuf[t] = (part * rz).astype(jnp.bfloat16)

    def remote(src, dst, send, recv, peer):
        return pltpu.make_async_remote_copy(src, dst, send, recv, device_id=peer, device_id_type=MESH)

    def d1(k):
        seqs = pl.ds(k * cs, cs)
        p = per_dev
        return (
            remote(sbuf.at[seqs, pl.ds(p, p)], r1.at[seqs, pl.ds(0, p)], s1_sem.at[k, 0], r1_sem.at[k, 0], core_peer),
            remote(sbuf.at[seqs, pl.ds(3 * p, p)], r1.at[seqs, pl.ds(p, p)], s1_sem.at[k, 1], r1_sem.at[k, 1], core_peer),
            remote(lse1.at[k], lr1.at[k], s1_sem.at[k, 2], r1_sem.at[k, 2], core_peer),
        )

    def d2(k):
        seqs = pl.ds(k * cs, cs)
        return (
            remote(s2.at[seqs], r2.at[seqs], s2_sem.at[k, 0], r2_sem.at[k, 0], x_peer),
            remote(lse2.at[k], lr2.at[k], s2_sem.at[k, 1], r2_sem.at[k, 1], x_peer),
        )

    def d3(k):
        seqs = pl.ds(k * cs, cs)
        return remote(xso.at[seqs], xs_hbm.at[pl.ds(m * n_half + k * cs, cs)], s3_sem.at[k], r3_sem.at[k], y_peer)

    def keep(k):
        seqs = pl.ds(k * cs, cs)
        return pltpu.make_async_copy(xso.at[seqs], xs_hbm.at[pl.ds(m * n_half + k * cs, cs)], osem.at[k])

    def weights(a, b):
        top = jnp.maximum(a, b)
        ea, eb = jnp.exp(a - top), jnp.exp(b - top)
        tot = ea + eb
        return jnp.transpose(ea / tot), jnp.transpose(eb / tot), top + jnp.log(tot)

    def merge1(k):
        for c in d1(k):
            c.wait_recv()
        p = per_dev
        wa, wb, joint = weights(lse1[k], pltpu.roll(lr1[k], n_slots - p, 1))
        lse2[k] = joint
        for j in range(cs):
            t = k * cs + j
            m0[t] = wa[:p, j:j + 1] * sbuf[t, 0:p, :].astype(jnp.float32) + wb[:p, j:j + 1] * r1[t, 0:p, :].astype(jnp.float32)
            s2[t] = (wa[2 * p:3 * p, j:j + 1] * sbuf[t, 2 * p:3 * p, :].astype(jnp.float32)
                     + wb[2 * p:3 * p, j:j + 1] * r1[t, p:2 * p, :].astype(jnp.float32)).astype(jnp.bfloat16)
        for c in d2(k):
            c.start()

    def merge2(k):
        for c in d2(k):
            c.wait_recv()
        p = per_dev
        wa, wb, _ = weights(lse2[k], pltpu.roll(lr2[k], n_slots - 2 * p, 1))
        for j in range(cs):
            t = k * cs + j
            xso[t] = (wa[:p, j:j + 1] * m0[t] + wb[:p, j:j + 1] * r2[t].astype(jnp.float32)).astype(jnp.bfloat16)
        d3(k).start()
        keep(k).start()

    early = n - LEAD
    late = min(LEAD, (steps - n) // LATE_EVERY)

    @pl.loop(0, steps)
    def _(k):
        @pl.when(k < n)
        def _():
            @pl.loop(0, cs)
            def _(j):
                own(k, j)

            for c in d1(k):
                c.start()

        @pl.when(k >= n)
        def _():
            @pl.loop(0, cs)
            def _(j):
                logits_and_mix(k * cs + j)

        @pl.when((k >= 1) & (k <= n))
        def _():
            merge1(k - 1)

        @pl.when((k >= LEAD) & (k < n))
        def _():
            merge2(k - LEAD)

        @pl.when((k >= n) & (lax.rem(k - n, LATE_EVERY) == 0) & ((k - n) // LATE_EVERY < late))
        def _():
            merge2(early + (k - n) // LATE_EVERY)

    @pl.loop(early + late, n)
    def _(k):
        merge2(k)

    @pl.loop(total - C_SLOTS, total)
    def _(t):
        c_copy(t).wait()

    @pl.loop(0, n)
    def _(k):
        for c in d1(k):
            c.wait_send()
        for c in d2(k):
            c.wait_send()
        d3(k).wait()
        keep(k).wait()


def dispatch(tokens, lengths, phi, scale, per_dev):
    batch, n_tok, dim = tokens.shape
    n_slots = phi.shape[1]
    half = batch // 2
    n = half // CHUNK_SEQS
    bf, f32 = jnp.bfloat16, jnp.float32
    return pl.pallas_call(
        functools.partial(dispatch_kernel, half, n_tok, n_slots, per_dev),
        out_shape=(jax.ShapeDtypeStruct((batch, per_dev, dim), bf), jax.ShapeDtypeStruct((batch, n_tok, n_slots), bf)),
        in_specs=[
            pl.BlockSpec(memory_space=pltpu.VMEM),
            pl.BlockSpec(memory_space=pltpu.SMEM),
            pl.BlockSpec(memory_space=pltpu.SMEM),
            pl.BlockSpec(memory_space=pl.ANY),
        ],
        out_specs=[pl.BlockSpec(memory_space=pl.ANY)] * 2,
        scratch_shapes=[
            pltpu.VMEM((dim, n_slots), bf),
            pltpu.VMEM((X_SLOTS, n_tok, dim), bf),
            pltpu.VMEM((n_tok, n_slots), f32),
            pltpu.VMEM((C_SLOTS, n_tok, n_slots), bf),
            pltpu.VMEM((half, n_slots, dim), bf),
            pltpu.VMEM((n, 8, n_slots), f32),
            pltpu.VMEM((half, 2 * per_dev, dim), bf),
            pltpu.VMEM((n, 8, n_slots), f32),
            pltpu.VMEM((half, per_dev, dim), f32),
            pltpu.VMEM((half, per_dev, dim), bf),
            pltpu.VMEM((n, 8, n_slots), f32),
            pltpu.VMEM((half, per_dev, dim), bf),
            pltpu.VMEM((n, 8, n_slots), f32),
            pltpu.VMEM((half, per_dev, dim), bf),
            pltpu.SemaphoreType.DMA((X_SLOTS,)),
            pltpu.SemaphoreType.DMA((C_SLOTS,)),
            pltpu.SemaphoreType.DMA((n,)),
            pltpu.SemaphoreType.DMA((n, 3)),
            pltpu.SemaphoreType.DMA((n, 3)),
            pltpu.SemaphoreType.DMA((n, 2)),
            pltpu.SemaphoreType.DMA((n, 2)),
            pltpu.SemaphoreType.DMA((n,)),
            pltpu.SemaphoreType.DMA((n,)),
        ],
        compiler_params=pltpu.CompilerParams(collective_id=0, has_side_effects=True, vmem_limit_bytes=58 * 1024 * 1024),
        name="dispatch",
    )(phi, lengths, scale, tokens)


def ffn_kernel(batch, slot_per, n_out, x_ref, wi_ref, wo_ref, *rest):
    outs, (xf, xe, acc, og, act) = rest[:n_out], rest[n_out:]
    e, h = pl.program_id(0), pl.program_id(1)
    last_e, last_h = pl.num_programs(0) - 1, pl.num_programs(1) - 1
    grp, dim = x_ref.shape[1:]
    tiles = dim // LANES

    @pl.when((e == 0) & (h == 0))
    def _():
        @pl.loop(0, batch, unroll=4)
        def _(b):
            rows = pl.ds(pl.multiple_of(b * grp, grp), grp)
            for c in range(tiles):
                xf[c, rows, :] = x_ref[b, :, c * LANES:(c + 1) * LANES].astype(jnp.float32)

    @pl.when(h == 0)
    def _():
        for q in range(slot_per):
            for c in range(tiles):
                rows = xf[c, pl.ds(e * slot_per + q, batch, stride=grp), :]
                xe[q * batch:(q + 1) * batch, c * LANES:(c + 1) * LANES] = rows.astype(jnp.bfloat16)

    hidden = wi_ref.shape[2]
    for i in range(0, hidden, 256):
        hid = jnp.dot(xe[...], wi_ref[0, :, i:i + 256], preferred_element_type=jnp.float32)
        act[:, i:i + 256] = (0.5 * hid * (1.0 + lax.erf(hid * 0.7071067811865476))).astype(jnp.bfloat16)
    for i in range(0, dim, 256):
        acc[:, i:i + 256] = jnp.where(h == 0, 0.0, acc[:, i:i + 256]) + jnp.dot(act[...], wo_ref[0, :, i:i + 256], preferred_element_type=jnp.float32)

    @pl.when(h == last_h)
    def _():
        for q in range(slot_per):
            for c in range(tiles):
                og[c, pl.ds(e * slot_per + q, batch, stride=grp), :] = acc[q * batch:(q + 1) * batch, c * LANES:(c + 1) * LANES]

    @pl.when((e == last_e) & (h == last_h))
    def _():
        step = batch // n_out
        for i, out in enumerate(outs):
            @pl.loop(0, step, unroll=4)
            def _(b):
                rows = pl.ds(pl.multiple_of((i * step + b) * grp, grp), grp)
                for c in range(tiles):
                    out[b, :, c * LANES:(c + 1) * LANES] = og[c, rows, :].astype(jnp.bfloat16)


def ffn(group, xs, w_in, w_out, slot_per):
    batch, _, dim = xs.shape
    experts, _, hidden = w_in.shape
    ge = experts // GROUPS
    grp = ge * slot_per
    first = group * ge
    n_out = CHUNKS[group]
    step = batch // n_out
    rows = batch * slot_per
    return pl.pallas_call(
        functools.partial(ffn_kernel, batch, slot_per, n_out),
        grid=(ge, hidden // HIDDEN_TILE),
        out_shape=[jax.ShapeDtypeStruct((step, grp, dim), jnp.bfloat16)] * n_out,
        in_specs=[
            pl.BlockSpec((batch, grp, dim), lambda e, h: (0, group, 0)),
            pl.BlockSpec((1, dim, HIDDEN_TILE), lambda e, h: (first + e, 0, h)),
            pl.BlockSpec((1, HIDDEN_TILE, dim), lambda e, h: (first + e, h, 0)),
        ],
        out_specs=[pl.BlockSpec((step, grp, dim), lambda e, h: (0, 0, 0))] * n_out,
        scratch_shapes=[
            pltpu.VMEM((dim // LANES, batch * grp, LANES), jnp.float32),
            pltpu.VMEM((rows, dim), jnp.bfloat16),
            pltpu.VMEM((rows, dim), jnp.float32),
            pltpu.VMEM((dim // LANES, batch * grp, LANES), jnp.float32),
            pltpu.VMEM((rows, HIDDEN_TILE), jnp.bfloat16),
        ],
        compiler_params=pltpu.CompilerParams(dimension_semantics=("arbitrary", "arbitrary"), vmem_limit_bytes=58 * 1024 * 1024),
        cost_estimate=pl.CostEstimate(flops=4 * ge * rows * dim * hidden, bytes_accessed=4 * ge * dim * hidden, transcendentals=0),
        name="ffn",
    )(xs, w_in, w_out)


def combine_kernel(first, n_tok, n_pieces, len_ref, off_ref, c_ref, *rest):
    pieces, out_ref = rest[:n_pieces], rest[-1]
    pos = off_ref[0] + lax.broadcasted_iota(jnp.int32, (n_tok, 1), 0)
    for i in range(COMBINE_SEQS):
        slots = jnp.concatenate([p[i] for p in pieces], axis=0)
        mixed = jnp.dot(c_ref[i], slots, preferred_element_type=jnp.float32)
        ok = pos < len_ref[first + pl.program_id(0) * COMBINE_SEQS + i]
        out_ref[i] = jnp.where(ok, mixed, 0.0).astype(jnp.bfloat16)


def combine(chunk, mix, pieces, lengths, offset, y):
    batch, n_tok, n_slots = mix.shape
    _, grp, dim = pieces[0][0].shape
    cs = COMBINE_SEQS
    step = batch // MIX_CHUNKS
    first = chunk * step
    n_p = len(pieces)
    base = first // cs
    in_specs = [
        pl.BlockSpec((cs, n_tok, n_slots), lambda b, *_: (base + b, 0, 0)),
        *[pl.BlockSpec((cs, grp, dim), functools.partial(lambda at, b, *_: (at // cs + b, 0, 0), at)) for _, at in pieces],
    ]
    pieces = [p for p, _ in pieces]
    args = [lengths, offset, mix, *pieces]
    alias = {}
    if y is not None:
        in_specs.append(pl.BlockSpec(memory_space=pl.ANY))
        args.append(y)
        alias = {len(args) - 1: 0}
    return pl.pallas_call(
        functools.partial(combine_kernel, first, n_tok, n_p),
        grid_spec=pltpu.PrefetchScalarGridSpec(
            num_scalar_prefetch=2,
            grid=(step // cs,),
            in_specs=in_specs,
            out_specs=pl.BlockSpec((cs, n_tok, dim), lambda b, *_: (base + b, 0, 0)),
        ),
        out_shape=jax.ShapeDtypeStruct((batch, n_tok, dim), jnp.bfloat16),
        input_output_aliases=alias,
        compiler_params=pltpu.CompilerParams(dimension_semantics=("arbitrary",), vmem_limit_bytes=32 * 1024 * 1024),
        cost_estimate=pl.CostEstimate(flops=2 * 2 * step * n_tok * n_slots * dim, bytes_accessed=2 * step * n_tok * (dim + n_slots), transcendentals=0),
        name="combine",
    )(*args)


def solution(mesh):
    seq_size = mesh.shape["seq"]
    swap_y = [(0, 1), (1, 0)]
    swap_x = [(i, i ^ 2) for i in range(seq_size)]
    swap_c = [(i, i ^ 1) for i in range(seq_size)]

    def local_layer(tokens, lengths, slot_params, logit_scale, w_in, w_out):
        n_tok = tokens.shape[1]
        per_dev = slot_params.shape[1] // seq_size
        slot_per = per_dev // w_in.shape[0]
        offset = (lax.axis_index("seq") * n_tok).reshape(1).astype(jnp.int32)
        xs, mix = dispatch(tokens, lengths, slot_params, logit_scale.reshape(1), per_dev)
        table = {}
        for group in range(GROUPS):
            parts = ffn(group, xs, w_in, w_out, slot_per)
            for k, part in enumerate(parts):
                other = lax.ppermute(part, "model", swap_y)
                own = (part.astype(jnp.float32) + other.astype(jnp.float32)).astype(jnp.bfloat16)
                across = lax.ppermute(own, "seq", swap_x)
                table[k, group, 0] = own
                table[k, group, 1] = lax.ppermute(own, "seq", swap_c)
                table[k, group, 2] = across
                table[k, group, 3] = lax.ppermute(across, "seq", swap_c)
        for part in range(MIX_CALLS):
            mix = mix_weights(part, tokens, lengths, slot_params, logit_scale.reshape(1), per_dev, mix)
        y = None
        for k in range(MIX_CHUNKS):
            pieces = []
            for q in range(seq_size):
                for group in range(GROUPS):
                    per = MIX_CHUNKS // CHUNKS[group]
                    pieces.append((table[k // per, group, q], k % per * (tokens.shape[0] // MIX_CHUNKS)))
            y = combine(k, mix, pieces, lengths, offset, y)
        return y


    return jax.shard_map(local_layer, mesh=mesh, in_specs=(P("data", "seq", None), P("data"), P(), P(), P("seq", None, "model"), P("seq", "model", None)), out_specs=P("data", "seq", None), check_vma=False)
```

```python
import functools

import jax
import jax.numpy as jnp
from jax import lax
from jax.experimental import pallas as pl
from jax.experimental.pallas import tpu as pltpu
from jax.sharding import PartitionSpec as P


NORM_EPS = 1e-6
NEG = -1e30
MESH = pl.DeviceIdType.MESH
CHUNK_SEQS = 2
LEAD = 4
LATE_EVERY = 1
IN_DISPATCH = 16
MIX_CALLS = 2
MIX_SEQS = 2
MIX_VMEM = 32
COMBINE_VMEM = 32
X_SLOTS = 6
C_SLOTS = 8
ROW_BLOCK = 256
HIDDEN_TILE = 2560
LANES = 128
GROUPS = 4
CHUNKS = (2, 2, 2, 4)
MIX_CHUNKS = 4
COMBINE_SEQS = 4


def slot_units(phi, s, per_dev):
    n_slots = phi.shape[1]
    p32 = phi.astype(jnp.float32)
    unit = (p32 * lax.rsqrt(jnp.sum(p32 * p32, axis=0, keepdims=True) + NORM_EPS)).astype(jnp.bfloat16)
    row = lax.broadcasted_iota(jnp.int32, (n_slots, n_slots), 0)
    col = lax.broadcasted_iota(jnp.int32, (n_slots, n_slots), 1)
    pick = jnp.where(row == jnp.bitwise_xor(col, s * per_dev), 1.0, 0.0).astype(jnp.bfloat16)
    return jnp.dot(unit, pick, preferred_element_type=jnp.float32).astype(jnp.bfloat16)


def logit_block(x_ref, dots, g, r):
    rows = pl.ds(r * ROW_BLOCK, ROW_BLOCK)
    square = jnp.zeros((ROW_BLOCK, LANES), jnp.float32)
    for c in range(x_ref.shape[1] // LANES):
        x32 = x_ref[rows, c * LANES:(c + 1) * LANES].astype(jnp.float32)
        square += x32 * x32
    scale = lax.rsqrt(jnp.sum(square, axis=1, keepdims=True) + NORM_EPS)
    return jnp.where(scale > 0.0, dots[r * ROW_BLOCK:(r + 1) * ROW_BLOCK] * (g * scale), 0.0)


def mix_block(lg, first_pos, length):
    e = jnp.exp(lg - jnp.max(lg, axis=1, keepdims=True))
    mix = e * (1.0 / jnp.sum(e, axis=1, keepdims=True))
    pos = first_pos + lax.broadcasted_iota(jnp.int32, (lg.shape[0], 1), 0)
    return jnp.where(pos < length, mix, 0.0).astype(jnp.bfloat16)


def mix_kernel(per_dev, seqs, idx_ref, len_ref, phi_ref, g_ref, x_ref, *rest):
    c_ref, v_ref = rest[-2:]
    s = idx_ref[0]
    i = pl.program_id(0)

    @pl.when(i == 0)
    def _():
        v_ref[...] = slot_units(phi_ref[...], s, per_dev)

    n_tok = x_ref.shape[1]
    for j in range(seqs):
        length = len_ref[(idx_ref[1] + i) * seqs + j]
        dots = jnp.dot(x_ref[j], v_ref[...], preferred_element_type=jnp.float32)
        for r in range(n_tok // ROW_BLOCK):
            lg = logit_block(x_ref.at[j], dots, g_ref[0], r)
            c_ref[j, r * ROW_BLOCK:(r + 1) * ROW_BLOCK, :] = mix_block(lg, s * n_tok + r * ROW_BLOCK, length)


def mix_weights(part, tokens, lengths, phi, scale, per_dev, mix):
    batch, n_tok, dim = tokens.shape
    n_slots = phi.shape[1]
    left = batch // 2 - IN_DISPATCH
    count = left // MIX_CALLS
    seqs = MIX_SEQS
    start = lax.rem(lax.axis_index("model") * (batch // 2) + batch // 2 + IN_DISPATCH + part * count, batch)
    index = jnp.stack([lax.axis_index("seq"), start // seqs]).astype(jnp.int32)
    first = part * count // seqs
    args = [index, lengths, phi, scale, tokens] + ([] if mix is None else [mix])
    return pl.pallas_call(
        functools.partial(mix_kernel, per_dev, seqs),
        grid_spec=pltpu.PrefetchScalarGridSpec(
            num_scalar_prefetch=2,
            grid=(count // seqs,),
            in_specs=[
                pl.BlockSpec((dim, n_slots), lambda i, *_: (0, 0)),
                pl.BlockSpec(memory_space=pltpu.SMEM),
                pl.BlockSpec((seqs, n_tok, dim), lambda i, idx, _: (idx[1] + i, 0, 0)),
            ] + ([] if mix is None else [pl.BlockSpec(memory_space=pl.ANY)]),
            out_specs=pl.BlockSpec((seqs, n_tok, n_slots), lambda i, *_: (first + i, 0, 0)),
            scratch_shapes=[pltpu.VMEM((dim, n_slots), jnp.bfloat16)],
        ),
        out_shape=jax.ShapeDtypeStruct((left, n_tok, n_slots), jnp.bfloat16),
        input_output_aliases={} if mix is None else {5: 0},
        compiler_params=pltpu.CompilerParams(dimension_semantics=("arbitrary",), vmem_limit_bytes=MIX_VMEM * 1024 * 1024),
        cost_estimate=pl.CostEstimate(flops=4 * count * n_tok * n_slots * dim, bytes_accessed=2 * count * n_tok * dim, transcendentals=0),
        name="mix",
    )(*args)


def dispatch_kernel(n_half, n_tok, n_slots, per_dev, phi_ref, len_ref, g_ref, x_hbm, xs_hbm, c_hbm,
                    v_ref, xbuf, lbuf, cbuf, sbuf, lse1, r1, lr1, m0, s2, lse2, r2, lr2, xso,
                    xsem, csem, osem, s1_sem, r1_sem, s2_sem, r2_sem, s3_sem, r3_sem):
    s = lax.axis_index("seq")
    m = lax.axis_index("model")
    core_peer = {"seq": s + 1 - 2 * lax.rem(s, 2)}
    x_peer = {"seq": lax.rem(s + 2, 4)}
    y_peer = {"model": 1 - m}
    cs = CHUNK_SEQS
    n = n_half // cs
    total = n_half + IN_DISPATCH
    steps = total // cs

    barrier = pltpu.get_barrier_semaphore()
    for peer in (core_peer, x_peer, y_peer):
        pl.semaphore_signal(barrier, inc=1, device_id=peer, device_id_type=MESH)

    def batch_of(t):
        return lax.rem(m * n_half + t, 2 * n_half)

    def x_copy(t):
        slot = lax.rem(t, X_SLOTS)
        return pltpu.make_async_copy(x_hbm.at[batch_of(t)], xbuf.at[slot], xsem.at[slot])

    def c_copy(t):
        slot = lax.rem(t, C_SLOTS)
        return pltpu.make_async_copy(cbuf.at[slot], c_hbm.at[batch_of(t)], csem.at[slot])

    for t in range(X_SLOTS - 1):
        x_copy(t).start()

    v_ref[...] = slot_units(phi_ref[...], s, per_dev)
    lse1[...] = jnp.zeros_like(lse1)
    g = g_ref[0]

    pl.semaphore_wait(barrier, 3)

    def logits_and_mix(t):
        xslot = lax.rem(t, X_SLOTS)
        cslot = lax.rem(t, C_SLOTS)
        length = len_ref[batch_of(t)]

        @pl.when(t + X_SLOTS - 1 < total)
        def _():
            x_copy(t + X_SLOTS - 1).start()

        x_copy(t).wait()

        @pl.when(t >= C_SLOTS)
        def _():
            c_copy(t - C_SLOTS).wait()

        dots = jnp.dot(xbuf[xslot], v_ref[...], preferred_element_type=jnp.float32)
        for r in range(n_tok // ROW_BLOCK):
            rows = pl.ds(r * ROW_BLOCK, ROW_BLOCK)
            lg = logit_block(xbuf.at[xslot], dots, g, r)
            lbuf[rows, :] = lg
            cbuf[cslot, rows, :] = mix_block(lg, s * n_tok + r * ROW_BLOCK, length)
        c_copy(t).start()
        return xslot, length

    def own(k, j):
        t = k * cs + j
        xslot, length = logits_and_mix(t)
        ok = s * n_tok + lax.broadcasted_iota(jnp.int32, (n_tok, 1), 0) < length
        lg = jnp.where(ok, lbuf[...], NEG)
        mx = jnp.max(lg, axis=0, keepdims=True)
        w = jnp.where(ok, jnp.exp(lg - mx), 0.0)
        z = jnp.sum(w, axis=0, keepdims=True)
        z = jnp.where(z > 0.0, z, 1.0)
        lse1[k, pl.ds(j, 1), :] = mx + jnp.log(z)
        rz = jnp.transpose(jnp.broadcast_to(1.0 / z, (8, n_slots)))[:, :1]
        part = lax.dot_general(w.astype(jnp.bfloat16), xbuf[xslot], (((0,), (0,)), ((), ())), preferred_element_type=jnp.float32)
        sbuf[t] = (part * rz).astype(jnp.bfloat16)

    def remote(src, dst, send, recv, peer):
        return pltpu.make_async_remote_copy(src, dst, send, recv, device_id=peer, device_id_type=MESH)

    def d1(k):
        seqs = pl.ds(k * cs, cs)
        p = per_dev
        return (
            remote(sbuf.at[seqs, pl.ds(p, p)], r1.at[seqs, pl.ds(0, p)], s1_sem.at[k, 0], r1_sem.at[k, 0], core_peer),
            remote(sbuf.at[seqs, pl.ds(3 * p, p)], r1.at[seqs, pl.ds(p, p)], s1_sem.at[k, 1], r1_sem.at[k, 1], core_peer),
            remote(lse1.at[k], lr1.at[k], s1_sem.at[k, 2], r1_sem.at[k, 2], core_peer),
        )

    def d2(k):
        seqs = pl.ds(k * cs, cs)
        return (
            remote(s2.at[seqs], r2.at[seqs], s2_sem.at[k, 0], r2_sem.at[k, 0], x_peer),
            remote(lse2.at[k], lr2.at[k], s2_sem.at[k, 1], r2_sem.at[k, 1], x_peer),
        )

    def d3(k):
        seqs = pl.ds(k * cs, cs)
        return remote(xso.at[seqs], xs_hbm.at[pl.ds(m * n_half + k * cs, cs)], s3_sem.at[k], r3_sem.at[k], y_peer)

    def keep(k):
        seqs = pl.ds(k * cs, cs)
        return pltpu.make_async_copy(xso.at[seqs], xs_hbm.at[pl.ds(m * n_half + k * cs, cs)], osem.at[k])

    def weights(a, b):
        top = jnp.maximum(a, b)
        ea, eb = jnp.exp(a - top), jnp.exp(b - top)
        tot = ea + eb
        return jnp.transpose(ea / tot), jnp.transpose(eb / tot), top + jnp.log(tot)

    def merge1(k):
        for c in d1(k):
            c.wait_recv()
        p = per_dev
        wa, wb, joint = weights(lse1[k], pltpu.roll(lr1[k], n_slots - p, 1))
        lse2[k] = joint
        for j in range(cs):
            t = k * cs + j
            m0[t] = wa[:p, j:j + 1] * sbuf[t, 0:p, :].astype(jnp.float32) + wb[:p, j:j + 1] * r1[t, 0:p, :].astype(jnp.float32)
            s2[t] = (wa[2 * p:3 * p, j:j + 1] * sbuf[t, 2 * p:3 * p, :].astype(jnp.float32)
                     + wb[2 * p:3 * p, j:j + 1] * r1[t, p:2 * p, :].astype(jnp.float32)).astype(jnp.bfloat16)
        for c in d2(k):
            c.start()

    def merge2(k):
        for c in d2(k):
            c.wait_recv()
        p = per_dev
        wa, wb, _ = weights(lse2[k], pltpu.roll(lr2[k], n_slots - 2 * p, 1))
        for j in range(cs):
            t = k * cs + j
            xso[t] = (wa[:p, j:j + 1] * m0[t] + wb[:p, j:j + 1] * r2[t].astype(jnp.float32)).astype(jnp.bfloat16)
        d3(k).start()
        keep(k).start()

    early = n - LEAD
    late = min(LEAD, (steps - n) // LATE_EVERY)

    @pl.loop(0, steps)
    def _(k):
        @pl.when(k < n)
        def _():
            @pl.loop(0, cs)
            def _(j):
                own(k, j)

            for c in d1(k):
                c.start()

        @pl.when(k >= n)
        def _():
            @pl.loop(0, cs)
            def _(j):
                logits_and_mix(k * cs + j)

        @pl.when((k >= 1) & (k <= n))
        def _():
            merge1(k - 1)

        @pl.when((k >= LEAD) & (k < n))
        def _():
            merge2(k - LEAD)

        @pl.when((k >= n) & (lax.rem(k - n, LATE_EVERY) == 0) & ((k - n) // LATE_EVERY < late))
        def _():
            merge2(early + (k - n) // LATE_EVERY)

    @pl.loop(early + late, n)
    def _(k):
        merge2(k)

    @pl.loop(total - C_SLOTS, total)
    def _(t):
        c_copy(t).wait()

    @pl.loop(0, n)
    def _(k):
        for c in d1(k):
            c.wait_send()
        for c in d2(k):
            c.wait_send()
        d3(k).wait()
        keep(k).wait()


def dispatch(tokens, lengths, phi, scale, per_dev):
    batch, n_tok, dim = tokens.shape
    n_slots = phi.shape[1]
    half = batch // 2
    n = half // CHUNK_SEQS
    bf, f32 = jnp.bfloat16, jnp.float32
    return pl.pallas_call(
        functools.partial(dispatch_kernel, half, n_tok, n_slots, per_dev),
        out_shape=(jax.ShapeDtypeStruct((batch, per_dev, dim), bf), jax.ShapeDtypeStruct((batch, n_tok, n_slots), bf)),
        in_specs=[
            pl.BlockSpec(memory_space=pltpu.VMEM),
            pl.BlockSpec(memory_space=pltpu.SMEM),
            pl.BlockSpec(memory_space=pltpu.SMEM),
            pl.BlockSpec(memory_space=pl.ANY),
        ],
        out_specs=[pl.BlockSpec(memory_space=pl.ANY)] * 2,
        scratch_shapes=[
            pltpu.VMEM((dim, n_slots), bf),
            pltpu.VMEM((X_SLOTS, n_tok, dim), bf),
            pltpu.VMEM((n_tok, n_slots), f32),
            pltpu.VMEM((C_SLOTS, n_tok, n_slots), bf),
            pltpu.VMEM((half, n_slots, dim), bf),
            pltpu.VMEM((n, 8, n_slots), f32),
            pltpu.VMEM((half, 2 * per_dev, dim), bf),
            pltpu.VMEM((n, 8, n_slots), f32),
            pltpu.VMEM((half, per_dev, dim), f32),
            pltpu.VMEM((half, per_dev, dim), bf),
            pltpu.VMEM((n, 8, n_slots), f32),
            pltpu.VMEM((half, per_dev, dim), bf),
            pltpu.VMEM((n, 8, n_slots), f32),
            pltpu.VMEM((half, per_dev, dim), bf),
            pltpu.SemaphoreType.DMA((X_SLOTS,)),
            pltpu.SemaphoreType.DMA((C_SLOTS,)),
            pltpu.SemaphoreType.DMA((n,)),
            pltpu.SemaphoreType.DMA((n, 3)),
            pltpu.SemaphoreType.DMA((n, 3)),
            pltpu.SemaphoreType.DMA((n, 2)),
            pltpu.SemaphoreType.DMA((n, 2)),
            pltpu.SemaphoreType.DMA((n,)),
            pltpu.SemaphoreType.DMA((n,)),
        ],
        compiler_params=pltpu.CompilerParams(collective_id=0, has_side_effects=True, vmem_limit_bytes=58 * 1024 * 1024),
        name="dispatch",
    )(phi, lengths, scale, tokens)


def ffn_kernel(batch, slot_per, n_out, x_ref, wi_ref, wo_ref, *rest):
    outs, (xf, xe, acc, og, act) = rest[:n_out], rest[n_out:]
    e, h = pl.program_id(0), pl.program_id(1)
    last_e, last_h = pl.num_programs(0) - 1, pl.num_programs(1) - 1
    grp, dim = x_ref.shape[1:]
    tiles = dim // LANES

    @pl.when((e == 0) & (h == 0))
    def _():
        @pl.loop(0, batch, unroll=4)
        def _(b):
            rows = pl.ds(pl.multiple_of(b * grp, grp), grp)
            for c in range(tiles):
                xf[c, rows, :] = x_ref[b, :, c * LANES:(c + 1) * LANES].astype(jnp.float32)

    @pl.when(h == 0)
    def _():
        for q in range(slot_per):
            for c in range(tiles):
                rows = xf[c, pl.ds(e * slot_per + q, batch, stride=grp), :]
                xe[q * batch:(q + 1) * batch, c * LANES:(c + 1) * LANES] = rows.astype(jnp.bfloat16)

    hidden = wi_ref.shape[2]
    for i in range(0, hidden, 256):
        hid = jnp.dot(xe[...], wi_ref[0, :, i:i + 256], preferred_element_type=jnp.float32)
        act[:, i:i + 256] = (0.5 * hid * (1.0 + lax.erf(hid * 0.7071067811865476))).astype(jnp.bfloat16)
    for i in range(0, dim, 256):
        acc[:, i:i + 256] = jnp.where(h == 0, 0.0, acc[:, i:i + 256]) + jnp.dot(act[...], wo_ref[0, :, i:i + 256], preferred_element_type=jnp.float32)

    @pl.when(h == last_h)
    def _():
        for q in range(slot_per):
            for c in range(tiles):
                og[c, pl.ds(e * slot_per + q, batch, stride=grp), :] = acc[q * batch:(q + 1) * batch, c * LANES:(c + 1) * LANES]

    @pl.when((e == last_e) & (h == last_h))
    def _():
        step = batch // n_out
        for i, out in enumerate(outs):
            @pl.loop(0, step, unroll=4)
            def _(b):
                rows = pl.ds(pl.multiple_of((i * step + b) * grp, grp), grp)
                for c in range(tiles):
                    out[b, :, c * LANES:(c + 1) * LANES] = og[c, rows, :].astype(jnp.bfloat16)


def ffn(group, xs, w_in, w_out, slot_per):
    batch, _, dim = xs.shape
    experts, _, hidden = w_in.shape
    ge = experts // GROUPS
    grp = ge * slot_per
    first = group * ge
    n_out = CHUNKS[group]
    step = batch // n_out
    rows = batch * slot_per
    return pl.pallas_call(
        functools.partial(ffn_kernel, batch, slot_per, n_out),
        grid=(ge, hidden // HIDDEN_TILE),
        out_shape=[jax.ShapeDtypeStruct((step, grp, dim), jnp.bfloat16)] * n_out,
        in_specs=[
            pl.BlockSpec((batch, grp, dim), lambda e, h: (0, group, 0)),
            pl.BlockSpec((1, dim, HIDDEN_TILE), lambda e, h: (first + e, 0, h)),
            pl.BlockSpec((1, HIDDEN_TILE, dim), lambda e, h: (first + e, h, 0)),
        ],
        out_specs=[pl.BlockSpec((step, grp, dim), lambda e, h: (0, 0, 0))] * n_out,
        scratch_shapes=[
            pltpu.VMEM((dim // LANES, batch * grp, LANES), jnp.float32),
            pltpu.VMEM((rows, dim), jnp.bfloat16),
            pltpu.VMEM((rows, dim), jnp.float32),
            pltpu.VMEM((dim // LANES, batch * grp, LANES), jnp.float32),
            pltpu.VMEM((rows, HIDDEN_TILE), jnp.bfloat16),
        ],
        compiler_params=pltpu.CompilerParams(dimension_semantics=("arbitrary", "arbitrary"), vmem_limit_bytes=58 * 1024 * 1024),
        cost_estimate=pl.CostEstimate(flops=4 * ge * rows * dim * hidden, bytes_accessed=4 * ge * dim * hidden, transcendentals=0),
        name="ffn",
    )(xs, w_in, w_out)


def combine_kernel(first, n_tok, n_pieces, extra, len_ref, off_ref, c_ref, *rest):
    pieces, out_ref = rest[extra:extra + n_pieces], rest[-1]
    pos = off_ref[0] + lax.broadcasted_iota(jnp.int32, (n_tok, 1), 0)
    for i in range(COMBINE_SEQS):
        slots = jnp.concatenate([p[i] for p in pieces], axis=0)
        mix = jnp.where(off_ref[1] == first, rest[0][i], c_ref[i]) if extra else c_ref[i]
        mixed = jnp.dot(mix, slots, preferred_element_type=jnp.float32)
        ok = pos < len_ref[first + pl.program_id(0) * COMBINE_SEQS + i]
        out_ref[i] = jnp.where(ok, mixed, 0.0).astype(jnp.bfloat16)


def combine(chunk, mix, left, pieces, lengths, offset, y):
    batch, n_tok, n_slots = mix.shape
    _, grp, dim = pieces[0][0].shape
    cs = COMBINE_SEQS
    step = batch // MIX_CHUNKS
    first = chunk * step
    n_p = len(pieces)
    base = first // cs
    in_specs = [
        pl.BlockSpec((cs, n_tok, n_slots), lambda b, *_: (base + b, 0, 0)),
        *([] if left is None else [pl.BlockSpec((cs, n_tok, n_slots), lambda b, *_: (b, 0, 0))]),
        *[pl.BlockSpec((cs, grp, dim), functools.partial(lambda at, b, *_: (at // cs + b, 0, 0), at)) for _, at in pieces],
    ]
    pieces = [p for p, _ in pieces]
    args = [lengths, offset, mix, *([] if left is None else [left]), *pieces]
    alias = {}
    if y is not None:
        in_specs.append(pl.BlockSpec(memory_space=pl.ANY))
        args.append(y)
        alias = {len(args) - 1: 0}
    return pl.pallas_call(
        functools.partial(combine_kernel, first, n_tok, n_p, 0 if left is None else 1),
        grid_spec=pltpu.PrefetchScalarGridSpec(
            num_scalar_prefetch=2,
            grid=(step // cs,),
            in_specs=in_specs,
            out_specs=pl.BlockSpec((cs, n_tok, dim), lambda b, *_: (base + b, 0, 0)),
        ),
        out_shape=jax.ShapeDtypeStruct((batch, n_tok, dim), jnp.bfloat16),
        input_output_aliases=alias,
        compiler_params=pltpu.CompilerParams(dimension_semantics=("arbitrary",), vmem_limit_bytes=COMBINE_VMEM * 1024 * 1024),
        cost_estimate=pl.CostEstimate(flops=2 * 2 * step * n_tok * n_slots * dim, bytes_accessed=2 * step * n_tok * (dim + n_slots), transcendentals=0),
        name="combine",
    )(*args)


def solution(mesh):
    seq_size = mesh.shape["seq"]
    swap_y = [(0, 1), (1, 0)]
    swap_x = [(i, i ^ 2) for i in range(seq_size)]
    swap_c = [(i, i ^ 1) for i in range(seq_size)]

    def local_layer(tokens, lengths, slot_params, logit_scale, w_in, w_out):
        n_tok = tokens.shape[1]
        per_dev = slot_params.shape[1] // seq_size
        slot_per = per_dev // w_in.shape[0]
        batch = tokens.shape[0]
        left_first = lax.rem(lax.axis_index("model") * (batch // 2) + batch // 2 + IN_DISPATCH, batch)
        offset = jnp.stack([lax.axis_index("seq") * n_tok, left_first]).astype(jnp.int32)
        xs, mix = dispatch(tokens, lengths, slot_params, logit_scale.reshape(1), per_dev)
        table = {}
        for group in range(GROUPS):
            parts = ffn(group, xs, w_in, w_out, slot_per)
            for k, part in enumerate(parts):
                other = lax.ppermute(part, "model", swap_y)
                own = (part.astype(jnp.float32) + other.astype(jnp.float32)).astype(jnp.bfloat16)
                across = lax.ppermute(own, "seq", swap_x)
                table[k, group, 0] = own
                table[k, group, 1] = lax.ppermute(own, "seq", swap_c)
                table[k, group, 2] = across
                table[k, group, 3] = lax.ppermute(across, "seq", swap_c)
        left = None
        for part in range(MIX_CALLS):
            left = mix_weights(part, tokens, lengths, slot_params, logit_scale.reshape(1), per_dev, left)
        y = None
        for k in range(MIX_CHUNKS):
            pieces = []
            for q in range(seq_size):
                for group in range(GROUPS):
                    per = MIX_CHUNKS // CHUNKS[group]
                    pieces.append((table[k // per, group, q], k % per * (tokens.shape[0] // MIX_CHUNKS)))
            y = combine(k, mix, left if k % 2 else None, pieces, lengths, offset, y)
        return y


    return jax.shard_map(local_layer, mesh=mesh, in_specs=(P("data", "seq", None), P("data"), P(), P(), P("seq", None, "model"), P("seq", "model", None)), out_specs=P("data", "seq", None), check_vma=False)
```
